32 devices in a mesh: rep: 4 (over z), data: 8 (over y, x, core).
Axes of the slice: x: 2, y: 2, z: 4, core: 2. Of those that a mesh axis runs over, the one named last changes fastest.
Arguments:
- x_in: bfloat16 [256, 32, 512], P(('rep', 'data'))
- d_out: float32 [256, 32, 512], P(('rep', 'data'))
- weights: bfloat16 [6, 1024, 2048], replicated
- biases: float32 [6, 2048], replicated
Outputs:
- output 1: float32 [6, 1024, 2048], replicated
- output 2: float32 [6, 2048], replicated
- output 3: float32 [256, 32, 512], P(('rep', 'data'))
All inputs are finite; a program needn't handle non-finite values.
Results may differ from the reference program's by a relative error of at most 0.00449199.
Values are sent between devices in bfloat16 or wider.
A program may use at most 1 GiB of HBM per device.

```python
import jax
import jax.numpy as jnp
from jax import lax

HIDDEN = 512
LAYERS = 6
BATCH = 256
SEQ = 32
BLOCK_ROWS = 8
NUM_BLOCKS = BATCH // BLOCK_ROWS


def setup_inputs(seed: int = 0) -> dict:
    key = jax.random.key(seed)
    k_x, k_dy, k_w, k_b = jax.random.split(key, 4)
    x_in = jax.random.normal(k_x, (BATCH, SEQ, HIDDEN), jnp.float32).astype(jnp.bfloat16)
    d_out = jax.random.normal(k_dy, (BATCH, SEQ, HIDDEN), jnp.float32)
    weights = (jax.random.normal(k_w, (LAYERS, 2 * HIDDEN, 4 * HIDDEN), jnp.float32) * (2 * HIDDEN) ** -0.5).astype(jnp.bfloat16)
    gate_shift = jnp.concatenate([jnp.zeros((HIDDEN,), jnp.float32), jnp.ones((HIDDEN,), jnp.float32), jnp.zeros((2 * HIDDEN,), jnp.float32)])
    biases = 0.5 * jax.random.normal(k_b, (LAYERS, 4 * HIDDEN), jnp.float32) + gate_shift
    return {'x_in': x_in, 'd_out': d_out, 'weights': weights, 'biases': biases}


def gate_values(z_all):
    hidden = z_all.shape[-1] // 4
    return (jax.nn.sigmoid(z_all[:, :hidden]), jax.nn.sigmoid(z_all[:, hidden:2 * hidden]),
            jnp.tanh(z_all[:, 2 * hidden:3 * hidden]), jax.nn.sigmoid(z_all[:, 3 * hidden:]))


def layer_forward(x_seq, w_layer, b_layer):
    w_rec = w_layer[HIDDEN:]
    x_proj = jnp.einsum('tbh,hg->tbg', x_seq.astype(jnp.float32), w_layer[:HIDDEN].astype(jnp.float32)) + b_layer

    def time_step(carry_in, step_in):
        h_prev, c_prev = carry_in
        z_in, x_t = step_in
        z_all = z_in + jnp.dot(h_prev, w_rec, preferred_element_type=jnp.float32)
        in_g, fg_g, cand_g, out_g = gate_values(z_all)
        c_new = fg_g * c_prev + in_g * cand_g
        h_new = out_g * jnp.tanh(c_new)
        h_low = h_new.astype(jnp.bfloat16)
        y_t = (h_new + x_t.astype(jnp.float32)).astype(jnp.bfloat16)
        return (h_low, c_new), (z_all, c_prev, h_low, y_t)

    init_state = (jnp.zeros((BLOCK_ROWS, HIDDEN), jnp.bfloat16), jnp.zeros((BLOCK_ROWS, HIDDEN), jnp.float32))
    _, (z_seq, c_prev_seq, h_seq, y_seq) = lax.scan(time_step, init_state, (x_proj, x_seq))
    return y_seq, (z_seq, c_prev_seq, h_seq)


def layer_backward(dy_seq, x_seq, w_layer, z_seq, c_prev_seq, h_seq):
    w_rec = w_layer[HIDDEN:]

    def time_step(carry_in, step_in):
        dh_rec, dc_next = carry_in
        dy_t, z_all, c_prev = step_in
        in_g, fg_g, cand_g, out_g = gate_values(z_all)
        tanh_c = jnp.tanh(fg_g * c_prev + in_g * cand_g)
        dh_tot = dy_t + dh_rec
        dc_tot = dc_next + dh_tot * out_g * (1.0 - tanh_c * tanh_c)
        dz_all = jnp.concatenate([dc_tot * cand_g * in_g * (1.0 - in_g),
                                  dc_tot * c_prev * fg_g * (1.0 - fg_g),
                                  dc_tot * in_g * (1.0 - cand_g * cand_g),
                                  dh_tot * tanh_c * out_g * (1.0 - out_g)], axis=-1)
        dz_low = dz_all.astype(jnp.bfloat16)
        dh_new = jnp.dot(dz_low, w_rec.T, preferred_element_type=jnp.float32)
        return (dh_new, dc_tot * fg_g), (dz_low, jnp.sum(dz_all, axis=0))

    zero_state = jnp.zeros((BLOCK_ROWS, HIDDEN), jnp.float32)
    _, (dz_seq, db_steps) = lax.scan(time_step, (zero_state, zero_state), (dy_seq, z_seq, c_prev_seq), reverse=True)
    dz_wide = dz_seq.astype(jnp.float32)
    dx_seq = dy_seq + jnp.einsum('tbg,hg->tbh', dz_wide, w_layer[:HIDDEN].astype(jnp.float32))
    dw_in = jnp.einsum('tbh,tbg->hg', x_seq.astype(jnp.float32), dz_wide)
    dw_rec = jnp.einsum('tbh,tbg->hg', h_seq[:-1].astype(jnp.float32), dz_wide[1:])
    return dx_seq, jnp.concatenate([dw_in, dw_rec], axis=0), jnp.sum(db_steps, axis=0)


def block_grads(x_blk, dy_blk, weights, biases):
    def forward_layer(x_cur, layer_params):
        y_seq, saved_acts = layer_forward(x_cur, layer_params[0], layer_params[1])
        return y_seq, (x_cur,) + saved_acts

    _, stored = lax.scan(forward_layer, jnp.swapaxes(x_blk, 0, 1), (weights, biases))

    def backward_layer(dy_cur, layer_data):
        w_layer, x_cur, z_seq, c_prev_seq, h_seq = layer_data
        dx_seq, dw_layer, db_layer = layer_backward(dy_cur, x_cur, w_layer, z_seq, c_prev_seq, h_seq)
        return dx_seq, (dw_layer, db_layer)

    dx_seq, (dw_all, db_all) = lax.scan(backward_layer, jnp.swapaxes(dy_blk, 0, 1), (weights,) + stored, reverse=True)
    return jnp.swapaxes(dx_seq, 0, 1), dw_all, db_all


def reference(x_in, d_out, weights, biases):
    x_blocks = x_in.reshape(NUM_BLOCKS, BLOCK_ROWS, SEQ, HIDDEN)
    dy_blocks = d_out.reshape(NUM_BLOCKS, BLOCK_ROWS, SEQ, HIDDEN)

    def block_body(grad_acc, block_in):
        dx_blk, dw_all, db_all = block_grads(block_in[0], block_in[1], weights, biases)
        return (grad_acc[0] + dw_all, grad_acc[1] + db_all), dx_blk

    init_acc = (jnp.zeros((LAYERS, 2 * HIDDEN, 4 * HIDDEN), jnp.float32), jnp.zeros((LAYERS, 4 * HIDDEN), jnp.float32))
    (dw_total, db_total), dx_blocks = lax.scan(block_body, init_acc, (x_blocks, dy_blocks))
    return dw_total, db_total, dx_blocks.reshape(BATCH, SEQ, HIDDEN)
```

```python
import functools

import jax
import jax.numpy as jnp
from jax import lax
from jax.experimental import pallas as pl
from jax.experimental.pallas import tpu as pltpu
from jax.sharding import PartitionSpec as P

MESH = pl.DeviceIdType.MESH
H = 512
G = 4 * H
T = 4
HB = 256


def sigmoid(z):
    return 0.5 * jnp.tanh(0.5 * z) + 0.5


def stack_kernel(steps, half, layers, x_ref, dy_ref, w_hbm, b_ref, dw_hbm, db_ref, dx_ref,
                 w, wt, xs, hs, gates, cs, xp, dzs, dys, xb, dyb, dxs, dr_s, dc_s, dbacc, xt, stage,
                 w_sem, in_send, in_recv, fsend, frecv, bsend, brecv, dx_send, dx_recv, out_sem):
    rows = 2 * half
    chunk = T * rows
    n_chunks = steps // T
    me = lax.axis_index("data")
    core = lax.rem(me, 2)
    partner = me + 1 - 2 * core
    first = core * layers

    barrier = pltpu.get_barrier_semaphore()
    pl.semaphore_signal(barrier, inc=1, device_id={"data": partner}, device_id_type=MESH)

    def weight_copy(l):
        return pltpu.make_async_copy(w_hbm.at[first + l], w.at[l], w_sem.at[l])

    for l in range(layers):
        weight_copy(l).start()
    pl.semaphore_wait(barrier, 1)

    def x_copy():
        return pltpu.make_async_remote_copy(src_ref=x_ref, dst_ref=xb, send_sem=in_send.at[0], recv_sem=in_recv.at[0],
                                            device_id={"data": partner}, device_id_type=MESH)

    def dy_copy():
        return pltpu.make_async_remote_copy(src_ref=dy_ref, dst_ref=dyb, send_sem=in_send.at[1], recv_sem=in_recv.at[1],
                                            device_id={"data": partner}, device_id_type=MESH)

    def chunk_rows(k):
        return pl.ds(pl.multiple_of(k * chunk, chunk), chunk)

    def f_copy(k):
        return pltpu.make_async_remote_copy(src_ref=xs.at[layers, chunk_rows(k)], dst_ref=xs.at[0, chunk_rows(k)],
                                            send_sem=fsend.at[k], recv_sem=frecv.at[k],
                                            device_id={"data": partner}, device_id_type=MESH)

    def b_copy(k):
        return pltpu.make_async_remote_copy(src_ref=dys.at[1, chunk_rows(k)], dst_ref=dys.at[0, chunk_rows(k)],
                                            send_sem=bsend.at[k], recv_sem=brecv.at[k],
                                            device_id={"data": partner}, device_id_type=MESH)

    def dx_copy():
        return pltpu.make_async_remote_copy(src_ref=dxs, dst_ref=dx_ref, send_sem=dx_send, recv_sem=dx_recv,
                                            device_id={"data": partner}, device_id_type=MESH)

    @pl.when(core == 1)
    def _():
        x_copy().start()

    @pl.when(core == 0)
    def _():
        dy_copy().start()

    for l in range(layers):
        hs[l, :rows, :] = jnp.zeros((rows, H), jnp.bfloat16)
        cs[l, :rows, :] = jnp.zeros((rows, H), jnp.float32)
    dr_s[...] = jnp.zeros_like(dr_s)
    dc_s[...] = jnp.zeros_like(dc_s)
    dbacc[...] = jnp.zeros_like(dbacc)

    @pl.when(core == 0)
    def _():
        x_copy().wait_recv()

        def join(t, carry):
            both = jnp.concatenate([x_ref[t].astype(jnp.float32), xb[t].astype(jnp.float32)], axis=0)
            xs[0, pl.ds(pl.multiple_of(t * rows, rows), rows), :] = both.astype(jnp.bfloat16)
            return carry

        lax.fori_loop(0, steps, join, 0)

    def fwd_layer(k, l):
        @pl.when(k == 0)
        def _():
            weight_copy(l).wait()

        bias = b_ref[pl.ds(first + l, 1), :]
        x_chunk = xs[l, chunk_rows(k), :]
        for q in range(4):
            cols = slice(q * H, (q + 1) * H)
            xp[:, cols] = jnp.dot(x_chunk, w[l, :H, cols], preferred_element_type=jnp.float32) + bias[:, cols]

        def step(s, carry):
            t = k * T + s
            now = pl.ds(pl.multiple_of(t * rows, rows), rows)
            nxt = pl.ds(pl.multiple_of(t * rows + rows, rows), rows)
            loc = pl.ds(pl.multiple_of(s * rows, rows), rows)
            h_prev = hs[l, now, :]
            for j in range(H // HB):
                part = []
                for q in range(4):
                    cols = slice(q * H + j * HB, q * H + (j + 1) * HB)
                    part.append(xp[loc, cols] + jnp.dot(h_prev, w[l, H:, cols], preferred_element_type=jnp.float32))
                hc = slice(j * HB, (j + 1) * HB)
                in_g, fg_g, cand_g, out_g = sigmoid(part[0]), sigmoid(part[1]), jnp.tanh(part[2]), sigmoid(part[3])
                c_new = fg_g * cs[l, now, hc] + in_g * cand_g
                h_new = out_g * jnp.tanh(c_new)
                cs[l, nxt, hc] = c_new
                hs[l, nxt, hc] = h_new.astype(jnp.bfloat16)
                xs[l + 1, now, hc] = (h_new + xs[l, now, hc].astype(jnp.float32)).astype(jnp.bfloat16)
                for q, gate in enumerate((in_g, fg_g, cand_g, out_g)):
                    gates[l, now, q * H + j * HB:q * H + (j + 1) * HB] = gate
            return carry

        lax.fori_loop(0, T, step, 0)

    def fwd_chunk(k, carry):
        @pl.when(core == 1)
        def _():
            f_copy(k).wait_recv()

        def layer(l, c):
            fwd_layer(k, l)
            return c

        lax.fori_loop(0, layers, layer, 0)

        @pl.when(core == 0)
        def _():
            f_copy(k).start()

        return carry

    lax.fori_loop(0, n_chunks, fwd_chunk, 0)

    def transpose_weights(i, carry):
        l = i // 8
        j = lax.rem(i, 8)
        cols = pl.ds(pl.multiple_of(j * 256, 256), 256)
        wt[l, cols, :] = w[l, :, cols].T
        return carry

    lax.fori_loop(0, layers * 8, transpose_weights, 0)

    @pl.when(core == 1)
    def _():
        dy_copy().wait_recv()

        def join(t, carry):
            dys[0, pl.ds(pl.multiple_of(t * rows, rows), rows), :] = jnp.concatenate([dyb[t], dy_ref[t]], axis=0)
            return carry

        lax.fori_loop(0, steps, join, 0)

    def bwd_layer(k, l, src):
        def step(i, carry):
            t = k * T + (T - 1 - i)
            now = pl.ds(pl.multiple_of(t * rows, rows), rows)
            nxt = pl.ds(pl.multiple_of(t * rows + rows, rows), rows)
            acc = jnp.zeros((rows, H), jnp.float32)
            for j in range(H // HB):
                hc = slice(j * HB, (j + 1) * HB)
                gc = [slice(q * H + j * HB, q * H + (j + 1) * HB) for q in range(4)]
                in_g, fg_g, cand_g, out_g = (gates[l, now, c] for c in gc)
                tanh_c = jnp.tanh(cs[l, nxt, hc])
                dh = dys[src, now, hc] + dr_s[l, :, hc]
                dc = dc_s[l, :, hc] + dh * out_g * (1.0 - tanh_c * tanh_c)
                dc_s[l, :, hc] = dc * fg_g
                dz = (dc * cand_g * in_g * (1.0 - in_g), dc * cs[l, now, hc] * fg_g * (1.0 - fg_g),
                      dc * in_g * (1.0 - cand_g * cand_g), dh * tanh_c * out_g * (1.0 - out_g))
                for q in range(4):
                    low = dz[q].astype(jnp.bfloat16)
                    dbacc[l, :, gc[q]] += dz[q]
                    dzs[l, now, gc[q]] = low
                    acc += jnp.dot(low, wt[l, gc[q], H:], preferred_element_type=jnp.float32)
            dr_s[l] = acc
            return carry

        lax.fori_loop(0, T, step, 0)
        r = chunk_rows(k)
        dys[1, r, :] = dys[src, r, :] + jnp.dot(dzs[l, r, :], wt[l, :, :H], preferred_element_type=jnp.float32)

    def bwd_chunk(i, carry):
        k = n_chunks - 1 - i

        @pl.when(core == 0)
        def _():
            b_copy(k).wait_recv()

        def layer(j, c):
            l = layers - 1 - j
            bwd_layer(k, l, jnp.minimum(j, 1))
            return c

        lax.fori_loop(0, layers, layer, 0)

        @pl.when(core == 1)
        def _():
            b_copy(k).start()

        return carry

    lax.fori_loop(0, n_chunks, bwd_chunk, 0)

    @pl.when(core == 0)
    def _():
        def split(t, carry):
            both = dys[1, pl.ds(pl.multiple_of(t * rows, rows), rows), :]
            dx_ref[t] = both[:half]
            dxs[t] = both[half:]
            return carry

        lax.fori_loop(0, steps, split, 0)
        dx_copy().start()

    for l in range(layers):
        db_ref[pl.ds(l, 1), :] = jnp.sum(dbacc[l], axis=0, keepdims=True)

    n_rows = steps * rows

    def out_copy(i):
        l = i // 4
        b = lax.rem(i, 4)
        return pltpu.make_async_copy(stage.at[lax.rem(i, 2)], dw_hbm.at[l, pl.ds(pl.multiple_of(b * 256, 256), 256)],
                                     out_sem.at[lax.rem(i, 2)])

    def dw_block(i, carry):
        l = i // 4
        b = lax.rem(i, 4)

        @pl.when(i >= 2)
        def _():
            out_copy(i - 2).wait()

        cols = pl.ds(pl.multiple_of(lax.rem(b, 2) * 256, 256), 256)

        @pl.when(b < 2)
        def _():
            xt[...] = xs[l, :, cols].T

        @pl.when(b >= 2)
        def _():
            xt[...] = hs[l, :n_rows, cols].T

        for q in range(4):
            stage[lax.rem(i, 2), :, q * H:(q + 1) * H] = jnp.dot(xt[...], dzs[l, :, q * H:(q + 1) * H],
                                                                preferred_element_type=jnp.float32)
        out_copy(i).start()
        return carry

    lax.fori_loop(0, layers * 4, dw_block, 0)
    out_copy(layers * 4 - 2).wait()
    out_copy(layers * 4 - 1).wait()

    @pl.when(core == 0)
    def _():
        dy_copy().wait_send()
        dx_copy().wait_send()

        def drain(k, carry):
            f_copy(k).wait_send()
            return carry

        lax.fori_loop(0, n_chunks, drain, 0)

    @pl.when(core == 1)
    def _():
        x_copy().wait_send()
        dx_copy().wait_recv()

        def drain(k, carry):
            b_copy(k).wait_send()
            return carry

        lax.fori_loop(0, n_chunks, drain, 0)


def run_stack(x_t, dy_t, weights, biases):
    steps, half, _ = x_t.shape
    layers = weights.shape[0] // 2
    rows = 2 * half
    n = steps * rows
    n_chunks = steps // T
    vmem = pl.BlockSpec(memory_space=pltpu.VMEM)
    hbm = pl.BlockSpec(memory_space=pl.ANY)
    bf, f32 = jnp.bfloat16, jnp.float32
    dma = pltpu.SemaphoreType.DMA
    return pl.pallas_call(
        functools.partial(stack_kernel, steps, half, layers),
        out_shape=(jax.ShapeDtypeStruct((layers, 2 * H, G), f32), jax.ShapeDtypeStruct((layers, G), f32),
                   jax.ShapeDtypeStruct((steps, half, H), f32)),
        in_specs=[vmem, vmem, hbm, vmem],
        out_specs=(hbm, vmem, vmem),
        scratch_shapes=[
            pltpu.VMEM((layers, 2 * H, G), bf), pltpu.VMEM((layers, G, 2 * H), bf),
            pltpu.VMEM((layers + 1, n, H), bf), pltpu.VMEM((layers, n + rows, H), bf),
            pltpu.VMEM((layers, n, G), f32), pltpu.VMEM((layers, n + rows, H), f32),
            pltpu.VMEM((T * rows, G), f32), pltpu.VMEM((layers, n, G), bf),
            pltpu.VMEM((2, n, H), f32), pltpu.VMEM((steps, half, H), bf),
            pltpu.VMEM((steps, half, H), f32), pltpu.VMEM((steps, half, H), f32),
            pltpu.VMEM((layers, rows, H), f32), pltpu.VMEM((layers, rows, H), f32),
            pltpu.VMEM((layers, rows, G), f32), pltpu.VMEM((256, n), bf), pltpu.VMEM((2, 256, G), f32),
            dma((layers,)), dma((2,)), dma((2,)), dma((n_chunks,)), dma((n_chunks,)), dma((n_chunks,)), dma((n_chunks,)),
            dma, dma, dma((2,)),
        ],
        compiler_params=pltpu.CompilerParams(collective_id=0, has_side_effects=True, vmem_limit_bytes=66_000_000),
        name="stack",
    )(x_t, dy_t, weights, biases)


def solution(mesh):
    batch_axes = tuple(mesh.axis_names)

    def device_step(x_in, d_out, weights, biases):
        dw, db, dx = run_stack(jnp.swapaxes(x_in, 0, 1), jnp.swapaxes(d_out, 0, 1), weights, biases)
        top = lax.rem(lax.axis_index("data"), 2) == 1
        dw_all = jnp.concatenate([jnp.where(top, 0.0, dw), jnp.where(top, dw, 0.0)])
        db_all = jnp.concatenate([jnp.where(top, 0.0, db), jnp.where(top, db, 0.0)])
        return lax.psum(dw_all, batch_axes), lax.psum(db_all, batch_axes), jnp.swapaxes(dx, 0, 1)

    return jax.shard_map(device_step, mesh=mesh,
                         in_specs=(P(batch_axes), P(batch_axes), P(), P()),
                         out_specs=(P(), P(), P(batch_axes)), check_vma=False)
```

```python
import functools

import jax
import jax.numpy as jnp
from jax import lax
from jax.experimental import pallas as pl
from jax.experimental.pallas import tpu as pltpu
from jax.sharding import PartitionSpec as P

MESH = pl.DeviceIdType.MESH
H = 512
G = 4 * H
T = 4
HB = 256


def sigmoid(z):
    return 0.5 * jnp.tanh(0.5 * z) + 0.5


def stack_kernel(steps, half, layers, x_ref, dy_ref, w_hbm, b_ref, dw_hbm, db_ref, dx_ref,
                 w, wt, xs, hs, gates, cs, xp, dzs, dys, xb, dyb, dxs, dr_s, dc_s, dbacc, xt, stage,
                 w_sem, in_send, in_recv, fsend, frecv, bsend, brecv, dx_send, dx_recv, out_sem):
    rows = 2 * half
    chunk = T * rows
    n_chunks = steps // T
    me = lax.axis_index("data")
    core = lax.rem(me, 2)
    partner = me + 1 - 2 * core
    first = core * layers

    barrier = pltpu.get_barrier_semaphore()
    pl.semaphore_signal(barrier, inc=1, device_id={"data": partner}, device_id_type=MESH)

    def weight_copy(l):
        return pltpu.make_async_copy(w_hbm.at[first + l], w.at[l], w_sem.at[l])

    for l in range(layers):
        weight_copy(l).start()
    pl.semaphore_wait(barrier, 1)

    def x_copy():
        return pltpu.make_async_remote_copy(src_ref=x_ref, dst_ref=xb, send_sem=in_send.at[0], recv_sem=in_recv.at[0],
                                            device_id={"data": partner}, device_id_type=MESH)

    def dy_copy():
        return pltpu.make_async_remote_copy(src_ref=dy_ref, dst_ref=dyb, send_sem=in_send.at[1], recv_sem=in_recv.at[1],
                                            device_id={"data": partner}, device_id_type=MESH)

    def chunk_rows(k):
        return pl.ds(pl.multiple_of(k * chunk, chunk), chunk)

    def f_copy(k):
        return pltpu.make_async_remote_copy(src_ref=xs.at[layers, chunk_rows(k)], dst_ref=xs.at[0, chunk_rows(k)],
                                            send_sem=fsend.at[k], recv_sem=frecv.at[k],
                                            device_id={"data": partner}, device_id_type=MESH)

    def b_copy(k):
        return pltpu.make_async_remote_copy(src_ref=dys.at[1, chunk_rows(k)], dst_ref=dys.at[0, chunk_rows(k)],
                                            send_sem=bsend.at[k], recv_sem=brecv.at[k],
                                            device_id={"data": partner}, device_id_type=MESH)

    def dx_copy():
        return pltpu.make_async_remote_copy(src_ref=dxs, dst_ref=dx_ref, send_sem=dx_send, recv_sem=dx_recv,
                                            device_id={"data": partner}, device_id_type=MESH)

    @pl.when(core == 1)
    def _():
        x_copy().start()

    @pl.when(core == 0)
    def _():
        dy_copy().start()

    for l in range(layers):
        hs[l, :rows, :] = jnp.zeros((rows, H), jnp.bfloat16)
        cs[l, :rows, :] = jnp.zeros((rows, H), jnp.float32)
    dr_s[...] = jnp.zeros_like(dr_s)
    dc_s[...] = jnp.zeros_like(dc_s)
    dbacc[...] = jnp.zeros_like(dbacc)

    @pl.when(core == 0)
    def _():
        x_copy().wait_recv()

        def join(t, carry):
            both = jnp.concatenate([x_ref[t].astype(jnp.float32), xb[t].astype(jnp.float32)], axis=0)
            xs[0, pl.ds(pl.multiple_of(t * rows, rows), rows), :] = both.astype(jnp.bfloat16)
            return carry

        lax.fori_loop(0, steps, join, 0)

    def fwd_layer(k, l):
        @pl.when(k == 0)
        def _():
            weight_copy(l).wait()

        bias = b_ref[pl.ds(first + l, 1), :]
        x_chunk = xs[l, chunk_rows(k), :]
        for q in range(4):
            cols = slice(q * H, (q + 1) * H)
            xp[:, cols] = jnp.dot(x_chunk, w[l, :H, cols], preferred_element_type=jnp.float32) + bias[:, cols]

        def step(s, carry):
            t = k * T + s
            now = pl.ds(pl.multiple_of(t * rows, rows), rows)
            nxt = pl.ds(pl.multiple_of(t * rows + rows, rows), rows)
            loc = pl.ds(pl.multiple_of(s * rows, rows), rows)
            h_prev = hs[l, now, :]
            for j in range(H // HB):
                part = []
                for q in range(4):
                    cols = slice(q * H + j * HB, q * H + (j + 1) * HB)
                    part.append(xp[loc, cols] + jnp.dot(h_prev, w[l, H:, cols], preferred_element_type=jnp.float32))
                hc = slice(j * HB, (j + 1) * HB)
                in_g, fg_g, cand_g, out_g = sigmoid(part[0]), sigmoid(part[1]), jnp.tanh(part[2]), sigmoid(part[3])
                c_new = fg_g * cs[l, now, hc] + in_g * cand_g
                h_new = out_g * jnp.tanh(c_new)
                cs[l, nxt, hc] = c_new
                hs[l, nxt, hc] = h_new.astype(jnp.bfloat16)
                xs[l + 1, now, hc] = (h_new + xs[l, now, hc].astype(jnp.float32)).astype(jnp.bfloat16)
                for q, gate in enumerate((in_g, fg_g, cand_g, out_g)):
                    gates[l, now, q * H + j * HB:q * H + (j + 1) * HB] = gate
            return carry

        lax.fori_loop(0, T, step, 0)

    def fwd_chunk(k, carry):
        @pl.when(core == 1)
        def _():
            f_copy(k).wait_recv()

        def layer(l, c):
            fwd_layer(k, l)
            return c

        lax.fori_loop(0, layers, layer, 0)

        @pl.when(core == 0)
        def _():
            f_copy(k).start()

        return carry

    lax.fori_loop(0, n_chunks, fwd_chunk, 0)

    def transpose_weights(i, carry):
        l = i // 8
        j = lax.rem(i, 8)
        cols = pl.ds(pl.multiple_of(j * 256, 256), 256)
        wt[l, cols, :] = w[l, :, cols].T
        return carry

    lax.fori_loop(0, layers * 8, transpose_weights, 0)

    @pl.when(core == 1)
    def _():
        dy_copy().wait_recv()

        def join(t, carry):
            dys[0, pl.ds(pl.multiple_of(t * rows, rows), rows), :] = jnp.concatenate([dyb[t], dy_ref[t]], axis=0)
            return carry

        lax.fori_loop(0, steps, join, 0)

    def bwd_layer(k, l, src):
        def step(i, carry):
            t = k * T + (T - 1 - i)
            now = pl.ds(pl.multiple_of(t * rows, rows), rows)
            nxt = pl.ds(pl.multiple_of(t * rows + rows, rows), rows)
            acc = jnp.zeros((rows, H), jnp.float32)
            for j in range(H // HB):
                hc = slice(j * HB, (j + 1) * HB)
                gc = [slice(q * H + j * HB, q * H + (j + 1) * HB) for q in range(4)]
                in_g, fg_g, cand_g, out_g = (gates[l, now, c] for c in gc)
                tanh_c = jnp.tanh(cs[l, nxt, hc])
                dh = dys[src, now, hc] + dr_s[l, :, hc]
                dc = dc_s[l, :, hc] + dh * out_g * (1.0 - tanh_c * tanh_c)
                dc_s[l, :, hc] = dc * fg_g
                dz = (dc * cand_g * in_g * (1.0 - in_g), dc * cs[l, now, hc] * fg_g * (1.0 - fg_g),
                      dc * in_g * (1.0 - cand_g * cand_g), dh * tanh_c * out_g * (1.0 - out_g))
                for q in range(4):
                    low = dz[q].astype(jnp.bfloat16)
                    dbacc[l, :, gc[q]] += dz[q]
                    dzs[l, now, gc[q]] = low
                    acc += jnp.dot(low, wt[l, gc[q], H:], preferred_element_type=jnp.float32)
            dr_s[l] = acc
            return carry

        lax.fori_loop(0, T, step, 0)
        r = chunk_rows(k)
        dys[1, r, :] = dys[src, r, :] + jnp.dot(dzs[l, r, :], wt[l, :, :H], preferred_element_type=jnp.float32)

    def bwd_chunk(i, carry):
        k = n_chunks - 1 - i

        @pl.when(core == 0)
        def _():
            b_copy(k).wait_recv()

        def layer(j, c):
            l = layers - 1 - j
            bwd_layer(k, l, jnp.minimum(j, 1))
            return c

        lax.fori_loop(0, layers, layer, 0)

        @pl.when(core == 1)
        def _():
            b_copy(k).start()

        return carry

    lax.fori_loop(0, n_chunks, bwd_chunk, 0)

    @pl.when(core == 0)
    def _():
        def split(t, carry):
            both = dys[1, pl.ds(pl.multiple_of(t * rows, rows), rows), :]
            dx_ref[t] = both[:half]
            dxs[t] = both[half:]
            return carry

        lax.fori_loop(0, steps, split, 0)
        dx_copy().start()

    db_ref[...] = jnp.zeros_like(db_ref)
    for l in range(layers):
        db_ref[pl.ds(l, 1), :] = jnp.sum(dbacc[l], axis=0, keepdims=True)

    n_rows = steps * rows

    def out_copy(i):
        l = i // 4
        b = lax.rem(i, 4)
        return pltpu.make_async_copy(stage.at[lax.rem(i, 2)], dw_hbm.at[l, pl.ds(pl.multiple_of(b * 256, 256), 256)],
                                     out_sem.at[lax.rem(i, 2)])

    def dw_block(i, carry):
        l = i // 4
        b = lax.rem(i, 4)

        @pl.when(i >= 2)
        def _():
            out_copy(i - 2).wait()

        cols = pl.ds(pl.multiple_of(lax.rem(b, 2) * 256, 256), 256)

        @pl.when(b < 2)
        def _():
            xt[...] = xs[l, :, cols].T

        @pl.when(b >= 2)
        def _():
            xt[...] = hs[l, :n_rows, cols].T

        for q in range(4):
            stage[lax.rem(i, 2), :, q * H:(q + 1) * H] = jnp.dot(xt[...], dzs[l, :, q * H:(q + 1) * H],
                                                                preferred_element_type=jnp.float32)
        out_copy(i).start()
        return carry

    lax.fori_loop(0, layers * 4, dw_block, 0)
    out_copy(layers * 4 - 2).wait()
    out_copy(layers * 4 - 1).wait()

    @pl.when(core == 0)
    def _():
        dy_copy().wait_send()
        dx_copy().wait_send()

        def drain(k, carry):
            f_copy(k).wait_send()
            return carry

        lax.fori_loop(0, n_chunks, drain, 0)

    @pl.when(core == 1)
    def _():
        x_copy().wait_send()
        dx_copy().wait_recv()

        def drain(k, carry):
            b_copy(k).wait_send()
            return carry

        lax.fori_loop(0, n_chunks, drain, 0)


def run_stack(x_t, dy_t, weights, biases):
    steps, half, _ = x_t.shape
    layers = weights.shape[0] // 2
    rows = 2 * half
    n = steps * rows
    n_chunks = steps // T
    vmem = pl.BlockSpec(memory_space=pltpu.VMEM)
    hbm = pl.BlockSpec(memory_space=pl.ANY)
    bf, f32 = jnp.bfloat16, jnp.float32
    dma = pltpu.SemaphoreType.DMA
    return pl.pallas_call(
        functools.partial(stack_kernel, steps, half, layers),
        out_shape=(jax.ShapeDtypeStruct((layers, 2 * H, G), f32), jax.ShapeDtypeStruct((8, G), f32),
                   jax.ShapeDtypeStruct((steps, half, H), f32)),
        in_specs=[vmem, vmem, hbm, vmem],
        out_specs=(hbm, vmem, vmem),
        scratch_shapes=[
            pltpu.VMEM((layers, 2 * H, G), bf), pltpu.VMEM((layers, G, 2 * H), bf),
            pltpu.VMEM((layers + 1, n, H), bf), pltpu.VMEM((layers, n + rows, H), bf),
            pltpu.VMEM((layers, n, G), f32), pltpu.VMEM((layers, n + rows, H), f32),
            pltpu.VMEM((T * rows, G), f32), pltpu.VMEM((layers, n, G), bf),
            pltpu.VMEM((2, n, H), f32), pltpu.VMEM((steps, half, H), bf),
            pltpu.VMEM((steps, half, H), f32), pltpu.VMEM((steps, half, H), f32),
            pltpu.VMEM((layers, rows, H), f32), pltpu.VMEM((layers, rows, H), f32),
            pltpu.VMEM((layers, rows, G), f32), pltpu.VMEM((256, n), bf), pltpu.VMEM((2, 256, G), f32),
            dma((layers,)), dma((2,)), dma((2,)), dma((n_chunks,)), dma((n_chunks,)), dma((n_chunks,)), dma((n_chunks,)),
            dma, dma, dma((2,)),
        ],
        compiler_params=pltpu.CompilerParams(collective_id=0, has_side_effects=True, vmem_limit_bytes=66_000_000),
        name="stack",
    )(x_t, dy_t, weights, biases)


BLOCKS = 4
ORDERS = ((("x", "y", "z1", "z2"),) * BLOCKS,
          (("y", "x", "z1", "z2"),) * BLOCKS,
          (("z1", "x", "y", "z2"), ("z1", "y", "x", "z2")) * (BLOCKS // 2))


def event_order(layers):
    free = {"x": 0.0, "y": 0.0, "z": 0.0}
    pending = []

    def send(now, c, s, step, dim, size):
        link = dim[0]
        start = max(now, free[link])
        free[link] = start + size * (1.5 if dim == "z2" else 1.0)
        pending.append((free[link] + 0.1, s, c, step))

    for s in range(BLOCKS):
        for c in range(layers):
            send(0.0, c, s, 0, ORDERS[c][s][0], 1.0)
    order = []
    while pending:
        pending.sort()
        now, s, c, step = pending.pop(0)
        order.append((c, s, step))
        if step < 7:
            p = step + 1 if step < 3 else 6 - step
            send(now, c, s, step + 1, ORDERS[c][s][p], 0.5 ** p)
    return order


def sum_kernel(layers, dw_in, db_in, dw_out, db_out, loc, land0, land1, land2, land3, dbl, dba,
               loc_sem, put_sem, rs_send, rs_recv, ag_send, ag_recv, c_send, c_recv, db_send, db_recv):
    land = (land0, land1, land2, land3)
    z = lax.axis_index("rep")
    d = lax.axis_index("data")
    core = lax.rem(d, 2)
    x_bit = lax.rem(d // 2, 2)
    y_bit = d // 4
    z1_bit = lax.rem(z, 2)
    z2_bit = z // 2
    bits = {"x": x_bit, "y": y_bit, "z1": z1_bit, "z2": z2_bit}
    peer = {"x": (z, d + 2 - 4 * x_bit), "y": (z, d + 4 - 8 * y_bit), "z1": (z + 1 - 2 * z1_bit, d),
            "z2": (z + 2 - 4 * z2_bit, d), "c": (z, d + 1 - 2 * core)}
    first = core * layers
    block = dw_in.shape[1] // BLOCKS

    barrier = pltpu.get_barrier_semaphore()
    for p in peer.values():
        pl.semaphore_signal(barrier, inc=1, device_id=p, device_id_type=MESH)
    pl.semaphore_wait(barrier, len(peer))

    def rows(off, size):
        return pl.ds(pl.multiple_of(off, 8), size)

    def offset(c, s, steps):
        off = s * block
        for p in range(steps):
            off = off + bits[ORDERS[c][s][p]] * (block >> (p + 1))
        return off

    def local_load(c, s):
        return pltpu.make_async_copy(dw_in.at[c, rows(offset(c, s, 1), block // 2)], loc.at[c, s], loc_sem.at[c, s])

    def reduce_copy(c, s, p):
        dim = ORDERS[c][s][p]
        size = block >> (p + 1)
        if p == 0:
            src = dw_in.at[c, rows(s * block + (1 - bits[dim]) * size, size)]
        else:
            src = land[p - 1].at[c, s, rows((1 - bits[dim]) * size, size)]
        return pltpu.make_async_remote_copy(src_ref=src, dst_ref=land[p].at[c, s], send_sem=rs_send.at[c, s, p],
                                            recv_sem=rs_recv.at[c, s, p], device_id=peer[dim], device_id_type=MESH)

    def put(c, s):
        return pltpu.make_async_copy(land3.at[c, s], dw_out.at[first + c, rows(offset(c, s, 4), block // 16)],
                                     put_sem.at[c, s])

    def gather_copy(c, s, p):
        dim = ORDERS[c][s][p]
        where = dw_out.at[first + c, rows(offset(c, s, p + 1), block >> (p + 1))]
        return pltpu.make_async_remote_copy(src_ref=land3.at[c, s] if p == 3 else where, dst_ref=where,
                                            send_sem=ag_send.at[c, s, p], recv_sem=ag_recv.at[c, s, p],
                                            device_id=peer[dim], device_id_type=MESH)

    def core_copy(c, s):
        where = dw_out.at[first + c, rows(s * block, block)]
        return pltpu.make_async_remote_copy(src_ref=where, dst_ref=where, send_sem=c_send.at[c, s],
                                            recv_sem=c_recv.at[c, s], device_id=peer["c"], device_id_type=MESH)

    db_dims = ("x", "y", "z1", "z2")

    def db_copy(p):
        return pltpu.make_async_remote_copy(src_ref=dba.at[p], dst_ref=dbl.at[p], send_sem=db_send.at[p],
                                            recv_sem=db_recv.at[p], device_id=peer[db_dims[p]], device_id_type=MESH)

    def db_core_copy():
        return pltpu.make_async_remote_copy(src_ref=dba.at[4], dst_ref=db_out.at[core], send_sem=db_send.at[4],
                                            recv_sem=db_recv.at[4], device_id=peer["c"], device_id_type=MESH)

    dba[0] = db_in[...]
    db_copy(0).start()
    for s in range(BLOCKS):
        for c in range(layers):
            reduce_copy(c, s, 0).start()
    for s in range(BLOCKS):
        for c in range(layers):
            local_load(c, s).start()

    def add(dst, src_of, size):
        step = 8 if size >= 8 else size

        def body(i, carry):
            r = pl.ds(pl.multiple_of(i * step, step), step)
            dst[r, :] = dst[r, :] + src_of(i * step, step)
            return carry

        lax.fori_loop(0, size // step, body, 0)

    order = event_order(layers)
    spread = max(1, len(order) // 8)
    for n, (c, s, step) in enumerate(order):
        if step < 4:
            size = block >> (step + 1)
            reduce_copy(c, s, step).wait_recv()
            if step == 0:
                local_load(c, s).wait()
                add(land0.at[c, s], lambda i, k: loc[c, s, rows(i, k), :], size)
            else:
                keep = bits[ORDERS[c][s][step]] * size
                add(land[step].at[c, s], lambda i, k: land[step - 1][c, s, rows(keep + i, k), :], size)
            if step < 3:
                reduce_copy(c, s, step + 1).start()
            else:
                put(c, s).start()
                gather_copy(c, s, 3).start()
        else:
            p = 7 - step
            if p == 3:
                put(c, s).wait()
            gather_copy(c, s, p).wait_recv()
            if p > 0:
                gather_copy(c, s, p - 1).start()
            else:
                core_copy(c, s).start()
        if n % spread == spread - 1 and n // spread < 4:
            p = n // spread
            db_copy(p).wait_recv()
            dba[p + 1] = dba[p] + dbl[p]
            if p < 3:
                db_copy(p + 1).start()
            else:
                db_core_copy().start()
                db_out[core] = dba[4]

    for s in range(BLOCKS):
        for c in range(layers):
            core_copy(c, s).wait_recv()
            core_copy(c, s).wait_send()
            for p in range(4):
                reduce_copy(c, s, p).wait_send()
                gather_copy(c, s, p).wait_send()
    db_core_copy().wait()
    for p in range(4):
        db_copy(p).wait_send()


def sum_over_chips(dw, db):
    layers, n_rows, n_cols = dw.shape
    block = n_rows // BLOCKS
    f32 = jnp.float32
    vmem = pl.BlockSpec(memory_space=pltpu.VMEM)
    hbm = pl.BlockSpec(memory_space=pl.ANY)
    dma = pltpu.SemaphoreType.DMA
    return pl.pallas_call(
        functools.partial(sum_kernel, layers),
        out_shape=(jax.ShapeDtypeStruct((2 * layers, n_rows, n_cols), f32), jax.ShapeDtypeStruct((2,) + db.shape, f32)),
        in_specs=[hbm, vmem],
        out_specs=(hbm, vmem),
        scratch_shapes=[
            pltpu.VMEM((layers, BLOCKS, block // 2, n_cols), f32), pltpu.VMEM((layers, BLOCKS, block // 2, n_cols), f32),
            pltpu.VMEM((layers, BLOCKS, block // 4, n_cols), f32), pltpu.VMEM((layers, BLOCKS, block // 8, n_cols), f32),
            pltpu.VMEM((layers, BLOCKS, block // 16, n_cols), f32),
            pltpu.VMEM((4,) + db.shape, f32), pltpu.VMEM((5,) + db.shape, f32),
            dma((layers, BLOCKS)), dma((layers, BLOCKS)), dma((layers, BLOCKS, 4)), dma((layers, BLOCKS, 4)),
            dma((layers, BLOCKS, 4)), dma((layers, BLOCKS, 4)), dma((layers, BLOCKS)), dma((layers, BLOCKS)),
            dma((5,)), dma((5,)),
        ],
        compiler_params=pltpu.CompilerParams(collective_id=1, has_side_effects=True, vmem_limit_bytes=66_000_000),
        name="sum",
    )(dw, db)


def solution(mesh):
    batch_axes = tuple(mesh.axis_names)

    def device_step(x_in, d_out, weights, biases):
        layers = weights.shape[0] // 2
        dw, db, dx = run_stack(jnp.swapaxes(x_in, 0, 1), jnp.swapaxes(d_out, 0, 1), weights, biases)
        dw_all, db_all = sum_over_chips(dw, db)
        return dw_all, db_all[:, :layers].reshape(biases.shape), jnp.swapaxes(dx, 0, 1)

    return jax.shard_map(device_step, mesh=mesh,
                         in_specs=(P(batch_axes), P(batch_axes), P(), P()),
                         out_specs=(P(), P(), P(batch_axes)), check_vma=False)
```

```python
import functools

import jax
import jax.numpy as jnp
from jax import lax
from jax.experimental import pallas as pl
from jax.experimental.pallas import tpu as pltpu
from jax.sharding import PartitionSpec as P

MESH = pl.DeviceIdType.MESH
H = 512
G = 4 * H
T = 4
HB = 256


def sigmoid(z):
    return 0.5 * jnp.tanh(0.5 * z) + 0.5


PAIR = ("x", "y", "z1")


def chip_map():
    z = lax.axis_index("rep")
    d = lax.axis_index("data")
    core = lax.rem(d, 2)
    bits = {"x": lax.rem(d // 2, 2), "y": d // 4, "z1": lax.rem(z, 2), "z2": z // 2}
    peers = {"x": (z, d + 2 - 4 * bits["x"]), "y": (z, d + 4 - 8 * bits["y"]), "z1": (z + 1 - 2 * bits["z1"], d),
             "z2": (z + 2 - 4 * bits["z2"], d), "c": (z, d + 1 - 2 * core)}
    return bits, peers, core


def stack_kernel(steps, half, layers, x_ref, dy_ref, w_hbm, b_ref, dw_hbm, db_ref, dx_ref,
                 w, wt, xs, hs, gates, cs, xp, dzs, dys, xb, dyb, dr_s, dc_s, dbacc, xt, stage, xs_p, hs_p, dzs_p,
                 w_sem, in_send, in_recv, fsend, frecv, bsend, brecv, dx_send, dx_recv, out_sem,
                 a_send, a_recv, z_send, z_recv):
    rows = 2 * half
    chunk = T * rows
    n_chunks = steps // T
    bits, peers, core = chip_map()
    partner = peers["c"]
    first = core * layers

    barrier = pltpu.get_barrier_semaphore()
    greet = [partner] + [peers[dim] for dim in PAIR]
    for p in greet:
        pl.semaphore_signal(barrier, inc=1, device_id=p, device_id_type=MESH)

    def weight_copy(l):
        return pltpu.make_async_copy(w_hbm.at[first + l], w.at[l], w_sem.at[l])

    for l in range(layers):
        weight_copy(l).start()
    pl.semaphore_wait(barrier, len(greet))

    def x_copy():
        return pltpu.make_async_remote_copy(src_ref=x_ref, dst_ref=xb, send_sem=in_send.at[0], recv_sem=in_recv.at[0],
                                            device_id=partner, device_id_type=MESH)

    def dy_copy():
        return pltpu.make_async_remote_copy(src_ref=dy_ref, dst_ref=dyb, send_sem=in_send.at[1], recv_sem=in_recv.at[1],
                                            device_id=partner, device_id_type=MESH)

    def chunk_rows(k):
        return pl.ds(pl.multiple_of(k * chunk, chunk), chunk)

    def f_copy(k):
        return pltpu.make_async_remote_copy(src_ref=xs.at[layers, chunk_rows(k)], dst_ref=xs.at[0, chunk_rows(k)],
                                            send_sem=fsend.at[k], recv_sem=frecv.at[k],
                                            device_id=partner, device_id_type=MESH)

    def b_copy(k):
        return pltpu.make_async_remote_copy(src_ref=dys.at[1, chunk_rows(k)], dst_ref=dys.at[0, chunk_rows(k)],
                                            send_sem=bsend.at[k], recv_sem=brecv.at[k],
                                            device_id=partner, device_id_type=MESH)

    def dx_copy():
        return pltpu.make_async_remote_copy(src_ref=dyb, dst_ref=dx_ref, send_sem=dx_send, recv_sem=dx_recv,
                                            device_id=partner, device_id_type=MESH)

    def act_copy(l, part):
        src, dst = ((xs, xs_p), (hs, hs_p))[part]
        return pltpu.make_async_remote_copy(src_ref=src.at[l, pl.ds(0, steps * rows)], dst_ref=dst.at[l],
                                            send_sem=a_send.at[l, part], recv_sem=a_recv.at[l, part],
                                            device_id=peers[PAIR[l]], device_id_type=MESH)

    def dz_copy(l, k):
        cols = pl.ds(pl.multiple_of((1 - bits[PAIR[l]]) * (G // 2), G // 2), G // 2)
        return pltpu.make_async_remote_copy(src_ref=dzs.at[l, chunk_rows(k), cols], dst_ref=dzs_p.at[l, chunk_rows(k)],
                                            send_sem=z_send.at[l, k], recv_sem=z_recv.at[l, k],
                                            device_id=peers[PAIR[l]], device_id_type=MESH)

    @pl.when(core == 1)
    def _():
        x_copy().start()

    @pl.when(core == 0)
    def _():
        dy_copy().start()

    for l in range(layers):
        hs[l, :rows, :] = jnp.zeros((rows, H), jnp.bfloat16)
        cs[l, :rows, :] = jnp.zeros((rows, H), jnp.float32)
    dr_s[...] = jnp.zeros_like(dr_s)
    dc_s[...] = jnp.zeros_like(dc_s)
    dbacc[...] = jnp.zeros_like(dbacc)

    @pl.when(core == 0)
    def _():
        x_copy().wait_recv()

        def join(t, carry):
            both = jnp.concatenate([x_ref[t].astype(jnp.float32), xb[t].astype(jnp.float32)], axis=0)
            xs[0, pl.ds(pl.multiple_of(t * rows, rows), rows), :] = both.astype(jnp.bfloat16)
            return carry

        lax.fori_loop(0, steps, join, 0)

    def fwd_layer(k, l):
        @pl.when(k == 0)
        def _():
            weight_copy(l).wait()

        bias = b_ref[pl.ds(first + l, 1), :]
        x_chunk = xs[l, chunk_rows(k), :]
        for q in range(4):
            cols = slice(q * H, (q + 1) * H)
            xp[:, cols] = jnp.dot(x_chunk, w[l, :H, cols], preferred_element_type=jnp.float32) + bias[:, cols]

        def step(s, carry):
            t = k * T + s
            now = pl.ds(pl.multiple_of(t * rows, rows), rows)
            nxt = pl.ds(pl.multiple_of(t * rows + rows, rows), rows)
            loc = pl.ds(pl.multiple_of(s * rows, rows), rows)
            h_prev = hs[l, now, :]
            for j in range(H // HB):
                part = []
                for q in range(4):
                    cols = slice(q * H + j * HB, q * H + (j + 1) * HB)
                    part.append(xp[loc, cols] + jnp.dot(h_prev, w[l, H:, cols], preferred_element_type=jnp.float32))
                hc = slice(j * HB, (j + 1) * HB)
                in_g, fg_g, cand_g, out_g = sigmoid(part[0]), sigmoid(part[1]), jnp.tanh(part[2]), sigmoid(part[3])
                c_new = fg_g * cs[l, now, hc] + in_g * cand_g
                h_new = out_g * jnp.tanh(c_new)
                cs[l, nxt, hc] = c_new
                hs[l, nxt, hc] = h_new.astype(jnp.bfloat16)
                xs[l + 1, now, hc] = (h_new + xs[l, now, hc].astype(jnp.float32)).astype(jnp.bfloat16)
                for q, gate in enumerate((in_g, fg_g, cand_g, out_g)):
                    gates[l, now, q * H + j * HB:q * H + (j + 1) * HB] = gate
            return carry

        lax.fori_loop(0, T, step, 0)

    def fwd_chunk(k, carry):
        @pl.when(core == 1)
        def _():
            f_copy(k).wait_recv()

        def layer(l, c):
            fwd_layer(k, l)
            return c

        lax.fori_loop(0, layers, layer, 0)

        @pl.when(core == 0)
        def _():
            f_copy(k).start()

        return carry

    lax.fori_loop(0, n_chunks, fwd_chunk, 0)

    for l in range(layers):
        for part in range(2):
            act_copy(l, part).start()

    def transpose_weights(i, carry):
        l = i // 8
        j = lax.rem(i, 8)
        cols = pl.ds(pl.multiple_of(j * 256, 256), 256)
        wt[l, cols, :] = w[l, :, cols].T
        return carry

    lax.fori_loop(0, layers * 8, transpose_weights, 0)

    @pl.when(core == 1)
    def _():
        dy_copy().wait_recv()

        def join(t, carry):
            dys[0, pl.ds(pl.multiple_of(t * rows, rows), rows), :] = jnp.concatenate([dyb[t], dy_ref[t]], axis=0)
            return carry

        lax.fori_loop(0, steps, join, 0)

    def bwd_layer(k, l, src):
        def step(i, carry):
            t = k * T + (T - 1 - i)
            now = pl.ds(pl.multiple_of(t * rows, rows), rows)
            nxt = pl.ds(pl.multiple_of(t * rows + rows, rows), rows)
            acc = jnp.zeros((rows, H), jnp.float32)
            for j in range(H // HB):
                hc = slice(j * HB, (j + 1) * HB)
                gc = [slice(q * H + j * HB, q * H + (j + 1) * HB) for q in range(4)]
                in_g, fg_g, cand_g, out_g = (gates[l, now, c] for c in gc)
                tanh_c = jnp.tanh(cs[l, nxt, hc])
                dh = dys[src, now, hc] + dr_s[l, :, hc]
                dc = dc_s[l, :, hc] + dh * out_g * (1.0 - tanh_c * tanh_c)
                dc_s[l, :, hc] = dc * fg_g
                dz = (dc * cand_g * in_g * (1.0 - in_g), dc * cs[l, now, hc] * fg_g * (1.0 - fg_g),
                      dc * in_g * (1.0 - cand_g * cand_g), dh * tanh_c * out_g * (1.0 - out_g))
                for q in range(4):
                    low = dz[q].astype(jnp.bfloat16)
                    dbacc[l, :, gc[q]] += dz[q]
                    dzs[l, now, gc[q]] = low
                    acc += jnp.dot(low, wt[l, gc[q], H:], preferred_element_type=jnp.float32)
            dr_s[l] = acc
            return carry

        lax.fori_loop(0, T, step, 0)
        r = chunk_rows(k)
        dys[1, r, :] = dys[src, r, :] + jnp.dot(dzs[l, r, :], wt[l, :, :H], preferred_element_type=jnp.float32)

    def bwd_chunk(i, carry):
        k = n_chunks - 1 - i

        @pl.when(core == 0)
        def _():
            b_copy(k).wait_recv()

        def layer(j, c):
            l = layers - 1 - j
            bwd_layer(k, l, jnp.minimum(j, 1))
            return c

        lax.fori_loop(0, layers, layer, 0)

        @pl.when(core == 1)
        def _():
            b_copy(k).start()

        for l in range(layers):
            dz_copy(l, k).start()

        return carry

    lax.fori_loop(0, n_chunks, bwd_chunk, 0)

    @pl.when(core == 0)
    def _():
        def split(t, carry):
            both = dys[1, pl.ds(pl.multiple_of(t * rows, rows), rows), :]
            dx_ref[t] = both[:half]
            dyb[t] = both[half:]
            return carry

        lax.fori_loop(0, steps, split, 0)
        dx_copy().start()

    db_ref[...] = jnp.zeros_like(db_ref)
    for l in range(layers):
        db_ref[pl.ds(l, 1), :] = jnp.sum(dbacc[l], axis=0, keepdims=True)

    n_rows = steps * rows

    n_out = 2 * H // 256

    def out_copy(l, b):
        slot = b % 2
        return pltpu.make_async_copy(stage.at[slot], dw_hbm.at[l, pl.ds(b * 256, 256)], out_sem.at[slot])

    for l in range(layers):
        own = pl.ds(pl.multiple_of(bits[PAIR[l]] * (G // 2), G // 2), G // 2)
        for part in range(2):
            act_copy(l, part).wait_recv()

        def arrived(k, carry):
            dz_copy(l, k).wait_recv()
            return carry

        lax.fori_loop(0, n_chunks, arrived, 0)
        for b in range(n_out):
            mine, theirs = ((xs, xs_p), (hs, hs_p))[b * 256 // H]
            cols = slice(b * 256 % H, b * 256 % H + 256)
            if l * n_out + b >= 2:
                out_copy(l if b >= 2 else l - 1, (b - 2) % n_out).wait()
            xt[:, :n_rows] = mine[l, :n_rows, cols].T
            xt[:, n_rows:] = theirs[l, :, cols].T
            stage[b % 2] = (jnp.dot(xt[:, :n_rows], dzs[l, :, own], preferred_element_type=jnp.float32)
                            + jnp.dot(xt[:, n_rows:], dzs_p[l], preferred_element_type=jnp.float32))
            out_copy(l, b).start()
    out_copy(layers - 1, n_out - 2).wait()
    out_copy(layers - 1, n_out - 1).wait()

    for l in range(layers):
        for part in range(2):
            act_copy(l, part).wait_send()

        def sent(k, carry):
            dz_copy(l, k).wait_send()
            return carry

        lax.fori_loop(0, n_chunks, sent, 0)

    @pl.when(core == 0)
    def _():
        dy_copy().wait_send()
        dx_copy().wait_send()

        def drain(k, carry):
            f_copy(k).wait_send()
            return carry

        lax.fori_loop(0, n_chunks, drain, 0)

    @pl.when(core == 1)
    def _():
        x_copy().wait_send()
        dx_copy().wait_recv()

        def drain(k, carry):
            b_copy(k).wait_send()
            return carry

        lax.fori_loop(0, n_chunks, drain, 0)


def run_stack(x_t, dy_t, weights, biases):
    steps, half, _ = x_t.shape
    layers = weights.shape[0] // 2
    rows = 2 * half
    n = steps * rows
    n_chunks = steps // T
    vmem = pl.BlockSpec(memory_space=pltpu.VMEM)
    hbm = pl.BlockSpec(memory_space=pl.ANY)
    bf, f32 = jnp.bfloat16, jnp.float32
    dma = pltpu.SemaphoreType.DMA
    return pl.pallas_call(
        functools.partial(stack_kernel, steps, half, layers),
        out_shape=(jax.ShapeDtypeStruct((layers, 2 * H, G // 2), f32), jax.ShapeDtypeStruct((8, G), f32),
                   jax.ShapeDtypeStruct((steps, half, H), f32)),
        in_specs=[vmem, vmem, hbm, vmem],
        out_specs=(hbm, vmem, vmem),
        scratch_shapes=[
            pltpu.VMEM((layers, 2 * H, G), bf), pltpu.VMEM((layers, G, 2 * H), bf),
            pltpu.VMEM((layers + 1, n, H), bf), pltpu.VMEM((layers, n + rows, H), bf),
            pltpu.VMEM((layers, n, G), f32), pltpu.VMEM((layers, n + rows, H), f32),
            pltpu.VMEM((T * rows, G), f32), pltpu.VMEM((layers, n, G), bf),
            pltpu.VMEM((2, n, H), f32), pltpu.VMEM((steps, half, H), bf),
            pltpu.VMEM((steps, half, H), f32),
            pltpu.VMEM((layers, rows, H), f32), pltpu.VMEM((layers, rows, H), f32),
            pltpu.VMEM((layers, rows, G), f32), pltpu.VMEM((256, 2 * n), bf), pltpu.VMEM((2, 256, G // 2), f32),
            pltpu.VMEM((layers, n, H), bf), pltpu.VMEM((layers, n, H), bf), pltpu.VMEM((layers, n, G // 2), bf),
            dma((layers,)), dma((2,)), dma((2,)), dma((n_chunks,)), dma((n_chunks,)), dma((n_chunks,)), dma((n_chunks,)),
            dma, dma, dma((2,)),
            dma((layers, 2)), dma((layers, 2)), dma((layers, n_chunks)), dma((layers, n_chunks)),
        ],
        compiler_params=pltpu.CompilerParams(collective_id=0, has_side_effects=True, vmem_limit_bytes=67_000_000),
        name="stack",
    )(x_t, dy_t, weights, biases)


BLOCKS = 8
ORDERS = ((("y", "z1", "z2"),) * BLOCKS,
          (("x", "z1", "z2"),) * BLOCKS,
          (("x", "y", "z2"), ("y", "x", "z2")) * (BLOCKS // 2))


def event_order(layers):
    free = {"x": 0.0, "y": 0.0, "z": 0.0}
    pending = []

    def send(now, c, s, step):
        q = step if step < 3 else 5 - step
        dim = PAIR[c] if step == 6 else ORDERS[c][s][q]
        link = dim[0]
        free[link] = max(now, free[link]) + 0.5 ** q * (1.5 if dim == "z2" else 1.0)
        pending.append((free[link] + 0.1, s, c, step))

    for s in range(BLOCKS):
        for c in range(layers):
            send(0.0, c, s, 0)
    order = []
    while pending:
        pending.sort()
        now, s, c, step = pending.pop(0)
        order.append((c, s, step))
        if step < 6:
            send(now, c, s, step + 1)
    return order


def sum_kernel(layers, dw_in, db_in, dw_out, db_out, loc, land0, land1, land2, dbl, dba,
               loc_sem, put_sem, rs_send, rs_recv, ag_send, ag_recv, c_send, c_recv, db_send, db_recv):
    land = (land0, land1, land2)
    bits, peer, core = chip_map()
    first = core * layers
    block = dw_in.shape[1] // BLOCKS
    width = dw_in.shape[2]

    barrier = pltpu.get_barrier_semaphore()
    for p in peer.values():
        pl.semaphore_signal(barrier, inc=1, device_id=p, device_id_type=MESH)
    pl.semaphore_wait(barrier, len(peer))

    def rows(off, size):
        return pl.ds(pl.multiple_of(off, 8), size)

    def own_cols(c):
        return pl.ds(pl.multiple_of(bits[PAIR[c]] * width, width), width)

    def offset(c, s, steps):
        off = s * block
        for q in range(steps):
            off = off + bits[ORDERS[c][s][q]] * (block >> (q + 1))
        return off

    def local_load(c, s):
        return pltpu.make_async_copy(dw_in.at[c, rows(offset(c, s, 1), block // 2)], loc.at[c, s], loc_sem.at[c, s])

    def reduce_copy(c, s, q):
        dim = ORDERS[c][s][q]
        size = block >> (q + 1)
        if q == 0:
            src = dw_in.at[c, rows(s * block + (1 - bits[dim]) * size, size)]
        else:
            src = land[q - 1].at[c, s, rows((1 - bits[dim]) * size, size)]
        return pltpu.make_async_remote_copy(src_ref=src, dst_ref=land[q].at[c, s], send_sem=rs_send.at[c, s, q],
                                            recv_sem=rs_recv.at[c, s, q], device_id=peer[dim], device_id_type=MESH)

    def put(c, s):
        return pltpu.make_async_copy(land2.at[c, s], dw_out.at[first + c, rows(offset(c, s, 3), block // 8), own_cols(c)],
                                     put_sem.at[c, s])

    def gather_copy(c, s, step):
        q = 5 - step
        dim = PAIR[c] if q < 0 else ORDERS[c][s][q]
        where = dw_out.at[first + c, rows(offset(c, s, q + 1), block >> (q + 1)), own_cols(c)]
        return pltpu.make_async_remote_copy(src_ref=land2.at[c, s] if q == 2 else where, dst_ref=where,
                                            send_sem=ag_send.at[c, s, step - 3], recv_sem=ag_recv.at[c, s, step - 3],
                                            device_id=peer[dim], device_id_type=MESH)

    def core_copy(c, s):
        where = dw_out.at[first + c, rows(s * block, block)]
        return pltpu.make_async_remote_copy(src_ref=where, dst_ref=where, send_sem=c_send.at[c, s],
                                            recv_sem=c_recv.at[c, s], device_id=peer["c"], device_id_type=MESH)

    db_dims = ("x", "y", "z1", "z2")

    def db_copy(p):
        return pltpu.make_async_remote_copy(src_ref=dba.at[p], dst_ref=dbl.at[p], send_sem=db_send.at[p],
                                            recv_sem=db_recv.at[p], device_id=peer[db_dims[p]], device_id_type=MESH)

    def db_core_copy():
        return pltpu.make_async_remote_copy(src_ref=dba.at[4], dst_ref=db_out.at[core], send_sem=db_send.at[4],
                                            recv_sem=db_recv.at[4], device_id=peer["c"], device_id_type=MESH)

    dba[0] = db_in[...]
    db_copy(0).start()
    for s in range(BLOCKS):
        for c in range(layers):
            reduce_copy(c, s, 0).start()
    for s in range(BLOCKS):
        for c in range(layers):
            local_load(c, s).start()

    def add(dst, src_of, size):
        def body(i, carry):
            r = pl.ds(pl.multiple_of(i * 8, 8), 8)
            dst[r, :] = dst[r, :] + src_of(i * 8)
            return carry

        lax.fori_loop(0, size // 8, body, 0)

    order = event_order(layers)
    spread = max(1, len(order) // 8)
    for n, (c, s, step) in enumerate(order):
        if step < 3:
            size = block >> (step + 1)
            reduce_copy(c, s, step).wait_recv()
            if step == 0:
                local_load(c, s).wait()
                add(land0.at[c, s], lambda i: loc[c, s, rows(i, 8), :], size)
            else:
                keep = bits[ORDERS[c][s][step]] * size
                add(land[step].at[c, s], lambda i: land[step - 1][c, s, rows(keep + i, 8), :], size)
            if step < 2:
                reduce_copy(c, s, step + 1).start()
            else:
                put(c, s).start()
                gather_copy(c, s, 3).start()
        else:
            if step == 3:
                put(c, s).wait()
            gather_copy(c, s, step).wait_recv()
            if step < 6:
                gather_copy(c, s, step + 1).start()
            else:
                core_copy(c, s).start()
        if n % spread == spread - 1 and n // spread < 4:
            p = n // spread
            db_copy(p).wait_recv()
            dba[p + 1] = dba[p] + dbl[p]
            if p < 3:
                db_copy(p + 1).start()
            else:
                db_core_copy().start()
                db_out[core] = dba[4]

    for s in range(BLOCKS):
        for c in range(layers):
            core_copy(c, s).wait_recv()
            core_copy(c, s).wait_send()
            for q in range(3):
                reduce_copy(c, s, q).wait_send()
            for step in range(3, 7):
                gather_copy(c, s, step).wait_send()
    db_core_copy().wait()
    for p in range(4):
        db_copy(p).wait_send()


def sum_over_chips(dw, db):
    layers, n_rows, n_cols = dw.shape
    block = n_rows // BLOCKS
    f32 = jnp.float32
    vmem = pl.BlockSpec(memory_space=pltpu.VMEM)
    hbm = pl.BlockSpec(memory_space=pl.ANY)
    dma = pltpu.SemaphoreType.DMA
    return pl.pallas_call(
        functools.partial(sum_kernel, layers),
        out_shape=(jax.ShapeDtypeStruct((2 * layers, n_rows, 2 * n_cols), f32), jax.ShapeDtypeStruct((2,) + db.shape, f32)),
        in_specs=[hbm, vmem],
        out_specs=(hbm, vmem),
        scratch_shapes=[
            pltpu.VMEM((layers, BLOCKS, block // 2, n_cols), f32), pltpu.VMEM((layers, BLOCKS, block // 2, n_cols), f32),
            pltpu.VMEM((layers, BLOCKS, block // 4, n_cols), f32), pltpu.VMEM((layers, BLOCKS, block // 8, n_cols), f32),
            pltpu.VMEM((4,) + db.shape, f32), pltpu.VMEM((5,) + db.shape, f32),
            dma((layers, BLOCKS)), dma((layers, BLOCKS)), dma((layers, BLOCKS, 3)), dma((layers, BLOCKS, 3)),
            dma((layers, BLOCKS, 4)), dma((layers, BLOCKS, 4)), dma((layers, BLOCKS)), dma((layers, BLOCKS)),
            dma((5,)), dma((5,)),
        ],
        compiler_params=pltpu.CompilerParams(collective_id=1, has_side_effects=True, vmem_limit_bytes=67_000_000),
        name="sum",
    )(dw, db)


def solution(mesh):
    batch_axes = tuple(mesh.axis_names)

    def device_step(x_in, d_out, weights, biases):
        layers = weights.shape[0] // 2
        dw, db, dx = run_stack(jnp.swapaxes(x_in, 0, 1), jnp.swapaxes(d_out, 0, 1), weights, biases)
        dw_all, db_all = sum_over_chips(dw, db)
        return dw_all, db_all[:, :layers].reshape(biases.shape), jnp.swapaxes(dx, 0, 1)

    return jax.shard_map(device_step, mesh=mesh,
                         in_specs=(P(batch_axes), P(batch_axes), P(), P()),
                         out_specs=(P(), P(), P(batch_axes)), check_vma=False)
```

```python
import functools

import jax
import jax.numpy as jnp
from jax import lax
from jax.experimental import pallas as pl
from jax.experimental.pallas import tpu as pltpu
from jax.sharding import PartitionSpec as P

MESH = pl.DeviceIdType.MESH
H = 512
G = 4 * H
T = 8
HB = 256


def sigmoid(z):
    return 0.5 * jnp.tanh(0.5 * z) + 0.5


PAIR = ("x", "y", "z1")


def chip_map():
    z = lax.axis_index("rep")
    d = lax.axis_index("data")
    core = lax.rem(d, 2)
    bits = {"x": lax.rem(d // 2, 2), "y": d // 4, "z1": lax.rem(z, 2), "z2": z // 2}
    peers = {"x": (z, d + 2 - 4 * bits["x"]), "y": (z, d + 4 - 8 * bits["y"]), "z1": (z + 1 - 2 * bits["z1"], d),
             "z2": (z + 2 - 4 * bits["z2"], d), "c": (z, d + 1 - 2 * core)}
    return bits, peers, core


def stack_kernel(steps, half, layers, x_ref, dy_ref, w_hbm, b_ref, dw_hbm, db_ref, dx_ref,
                 w, wt, xs, hs, gates, cs, xp, dzs, dys, xb, dyb, dr_s, dc_s, dbacc, xt, stage, xs_p, hs_p, dzs_p,
                 w_sem, in_send, in_recv, fsend, frecv, bsend, brecv, dx_send, dx_recv, out_sem,
                 a_send, a_recv, z_send, z_recv):
    rows = 2 * half
    chunk = T * rows
    n_chunks = steps // T
    bits, peers, core = chip_map()
    partner = peers["c"]
    first = core * layers

    barrier = pltpu.get_barrier_semaphore()
    greet = [partner] + [peers[dim] for dim in PAIR]
    for p in greet:
        pl.semaphore_signal(barrier, inc=1, device_id=p, device_id_type=MESH)

    def weight_copy(l):
        return pltpu.make_async_copy(w_hbm.at[first + l], w.at[l], w_sem.at[l])

    for l in range(layers):
        weight_copy(l).start()
    pl.semaphore_wait(barrier, len(greet))

    def x_copy():
        return pltpu.make_async_remote_copy(src_ref=x_ref, dst_ref=xb, send_sem=in_send.at[0], recv_sem=in_recv.at[0],
                                            device_id=partner, device_id_type=MESH)

    def dy_copy():
        return pltpu.make_async_remote_copy(src_ref=dy_ref, dst_ref=dyb, send_sem=in_send.at[1], recv_sem=in_recv.at[1],
                                            device_id=partner, device_id_type=MESH)

    def chunk_rows(k):
        return pl.ds(pl.multiple_of(k * chunk, chunk), chunk)

    def f_copy(k):
        return pltpu.make_async_remote_copy(src_ref=xs.at[layers, chunk_rows(k)], dst_ref=xs.at[0, chunk_rows(k)],
                                            send_sem=fsend.at[k], recv_sem=frecv.at[k],
                                            device_id=partner, device_id_type=MESH)

    def b_copy(k):
        return pltpu.make_async_remote_copy(src_ref=dys.at[1, chunk_rows(k)], dst_ref=dys.at[0, chunk_rows(k)],
                                            send_sem=bsend.at[k], recv_sem=brecv.at[k],
                                            device_id=partner, device_id_type=MESH)

    def dx_copy():
        return pltpu.make_async_remote_copy(src_ref=dyb, dst_ref=dx_ref, send_sem=dx_send, recv_sem=dx_recv,
                                            device_id=partner, device_id_type=MESH)

    def act_copy(l, part):
        src, dst = ((xs, xs_p), (hs, hs_p))[part]
        return pltpu.make_async_remote_copy(src_ref=src.at[l, pl.ds(0, steps * rows)], dst_ref=dst.at[l],
                                            send_sem=a_send.at[l, part], recv_sem=a_recv.at[l, part],
                                            device_id=peers[PAIR[l]], device_id_type=MESH)

    def dz_copy(l, k):
        cols = pl.ds(pl.multiple_of((1 - bits[PAIR[l]]) * (G // 2), G // 2), G // 2)
        return pltpu.make_async_remote_copy(src_ref=dzs.at[l, chunk_rows(k), cols], dst_ref=dzs_p.at[l, chunk_rows(k)],
                                            send_sem=z_send.at[l, k], recv_sem=z_recv.at[l, k],
                                            device_id=peers[PAIR[l]], device_id_type=MESH)

    @pl.when(core == 1)
    def _():
        x_copy().start()

    @pl.when(core == 0)
    def _():
        dy_copy().start()

    for l in range(layers):
        hs[l, :rows, :] = jnp.zeros((rows, H), jnp.bfloat16)
        cs[l, :rows, :] = jnp.zeros((rows, H), jnp.float32)
    dr_s[...] = jnp.zeros_like(dr_s)
    dc_s[...] = jnp.zeros_like(dc_s)
    dbacc[...] = jnp.zeros_like(dbacc)

    @pl.when(core == 0)
    def _():
        x_copy().wait_recv()

        def join(t, carry):
            both = jnp.concatenate([x_ref[t].astype(jnp.float32), xb[t].astype(jnp.float32)], axis=0)
            xs[0, pl.ds(pl.multiple_of(t * rows, rows), rows), :] = both.astype(jnp.bfloat16)
            return carry

        lax.fori_loop(0, steps, join, 0)

    def transpose_weights(i, carry):
        l = i // 8
        j = lax.rem(i, 8)
        cols = pl.ds(pl.multiple_of(j * 256, 256), 256)
        wt[l, cols, :] = w[l, :, cols].T
        return carry

    @pl.when(core == 1)
    def _():
        for l in range(layers):
            weight_copy(l).wait()
        lax.fori_loop(0, layers * 8, transpose_weights, 0)

    @pl.when(core == 1)
    def _():
        dy_copy().wait_recv()

        def join(t, carry):
            dys[0, pl.ds(pl.multiple_of(t * rows, rows), rows), :] = jnp.concatenate([dyb[t], dy_ref[t]], axis=0)
            return carry

        lax.fori_loop(0, steps, join, 0)

    def fwd_layer(k, l):
        @pl.when((k == 0) & (core == 0))
        def _():
            weight_copy(l).wait()

        bias = b_ref[pl.ds(first + l, 1), :]
        x_chunk = xs[l, chunk_rows(k), :]
        for q in range(4):
            cols = slice(q * H, (q + 1) * H)
            xp[:, cols] = jnp.dot(x_chunk, w[l, :H, cols], preferred_element_type=jnp.float32) + bias[:, cols]

        def step(s, carry):
            t = k * T + s
            now = pl.ds(pl.multiple_of(t * rows, rows), rows)
            nxt = pl.ds(pl.multiple_of(t * rows + rows, rows), rows)
            loc = pl.ds(pl.multiple_of(s * rows, rows), rows)
            h_prev = hs[l, now, :]
            for j in range(H // HB):
                part = []
                for q in range(4):
                    cols = slice(q * H + j * HB, q * H + (j + 1) * HB)
                    part.append(xp[loc, cols] + jnp.dot(h_prev, w[l, H:, cols], preferred_element_type=jnp.float32))
                hc = slice(j * HB, (j + 1) * HB)
                in_g, fg_g, cand_g, out_g = sigmoid(part[0]), sigmoid(part[1]), jnp.tanh(part[2]), sigmoid(part[3])
                c_new = fg_g * cs[l, now, hc] + in_g * cand_g
                h_new = out_g * jnp.tanh(c_new)
                cs[l, nxt, hc] = c_new
                hs[l, nxt, hc] = h_new.astype(jnp.bfloat16)
                xs[l + 1, now, hc] = (h_new + xs[l, now, hc].astype(jnp.float32)).astype(jnp.bfloat16)
                for q, gate in enumerate((in_g, fg_g, cand_g, out_g)):
                    gates[l, now, q * H + j * HB:q * H + (j + 1) * HB] = gate
            return carry

        lax.fori_loop(0, T, step, 0)

    def fwd_chunk(k, carry):
        @pl.when(core == 1)
        def _():
            f_copy(k).wait_recv()

        def layer(l, c):
            fwd_layer(k, l)
            return c

        lax.fori_loop(0, layers, layer, 0)

        @pl.when(core == 0)
        def _():
            f_copy(k).start()

        return carry

    lax.fori_loop(0, n_chunks, fwd_chunk, 0)

    for l in range(layers):
        for part in range(2):
            act_copy(l, part).start()

    @pl.when(core == 0)
    def _():
        lax.fori_loop(0, layers * 8, transpose_weights, 0)

    def bwd_layer(k, l, src):
        def step(i, carry):
            t = k * T + (T - 1 - i)
            now = pl.ds(pl.multiple_of(t * rows, rows), rows)
            nxt = pl.ds(pl.multiple_of(t * rows + rows, rows), rows)
            acc = jnp.zeros((rows, H), jnp.float32)
            for j in range(H // HB):
                hc = slice(j * HB, (j + 1) * HB)
                gc = [slice(q * H + j * HB, q * H + (j + 1) * HB) for q in range(4)]
                in_g, fg_g, cand_g, out_g = (gates[l, now, c] for c in gc)
                tanh_c = jnp.tanh(cs[l, nxt, hc])
                dh = dys[src, now, hc] + dr_s[l, :, hc]
                dc = dc_s[l, :, hc] + dh * out_g * (1.0 - tanh_c * tanh_c)
                dc_s[l, :, hc] = dc * fg_g
                dz = (dc * cand_g * in_g * (1.0 - in_g), dc * cs[l, now, hc] * fg_g * (1.0 - fg_g),
                      dc * in_g * (1.0 - cand_g * cand_g), dh * tanh_c * out_g * (1.0 - out_g))
                for q in range(4):
                    low = dz[q].astype(jnp.bfloat16)
                    dbacc[l, :, gc[q]] += dz[q]
                    dzs[l, now, gc[q]] = low
                    acc += jnp.dot(low, wt[l, gc[q], H:], preferred_element_type=jnp.float32)
            dr_s[l] = acc
            return carry

        lax.fori_loop(0, T, step, 0)
        r = chunk_rows(k)
        dys[1, r, :] = dys[src, r, :] + jnp.dot(dzs[l, r, :], wt[l, :, :H], preferred_element_type=jnp.float32)

    def bwd_chunk(i, carry):
        k = n_chunks - 1 - i

        @pl.when(core == 0)
        def _():
            b_copy(k).wait_recv()

        def layer(j, c):
            l = layers - 1 - j
            bwd_layer(k, l, jnp.minimum(j, 1))
            return c

        lax.fori_loop(0, layers, layer, 0)

        @pl.when(core == 1)
        def _():
            b_copy(k).start()

        for l in range(layers):
            dz_copy(l, k).start()

        return carry

    lax.fori_loop(0, n_chunks, bwd_chunk, 0)

    @pl.when(core == 0)
    def _():
        def split(t, carry):
            both = dys[1, pl.ds(pl.multiple_of(t * rows, rows), rows), :]
            dx_ref[t] = both[:half]
            dyb[t] = both[half:]
            return carry

        lax.fori_loop(0, steps, split, 0)
        dx_copy().start()

    db_ref[...] = jnp.zeros_like(db_ref)
    for l in range(layers):
        db_ref[pl.ds(l, 1), :] = jnp.sum(dbacc[l], axis=0, keepdims=True)

    n_rows = steps * rows

    n_out = 2 * H // 256

    def out_copy(l, b):
        slot = b % 2
        return pltpu.make_async_copy(stage.at[slot], dw_hbm.at[l, pl.ds(b * 256, 256)], out_sem.at[slot])

    for l in range(layers):
        own = pl.ds(pl.multiple_of(bits[PAIR[l]] * (G // 2), G // 2), G // 2)
        for part in range(2):
            act_copy(l, part).wait_recv()

        def arrived(k, carry):
            dz_copy(l, k).wait_recv()
            return carry

        lax.fori_loop(0, n_chunks, arrived, 0)
        for b in range(n_out):
            mine, theirs = ((xs, xs_p), (hs, hs_p))[b * 256 // H]
            cols = slice(b * 256 % H, b * 256 % H + 256)
            if l * n_out + b >= 2:
                out_copy(l if b >= 2 else l - 1, (b - 2) % n_out).wait()
            xt[:, :n_rows] = mine[l, :n_rows, cols].T
            xt[:, n_rows:] = theirs[l, :, cols].T
            stage[b % 2] = (jnp.dot(xt[:, :n_rows], dzs[l, :, own], preferred_element_type=jnp.float32)
                            + jnp.dot(xt[:, n_rows:], dzs_p[l], preferred_element_type=jnp.float32))
            out_copy(l, b).start()
    out_copy(layers - 1, n_out - 2).wait()
    out_copy(layers - 1, n_out - 1).wait()

    for l in range(layers):
        for part in range(2):
            act_copy(l, part).wait_send()

        def sent(k, carry):
            dz_copy(l, k).wait_send()
            return carry

        lax.fori_loop(0, n_chunks, sent, 0)

    @pl.when(core == 0)
    def _():
        dy_copy().wait_send()
        dx_copy().wait_send()

        def drain(k, carry):
            f_copy(k).wait_send()
            return carry

        lax.fori_loop(0, n_chunks, drain, 0)

    @pl.when(core == 1)
    def _():
        x_copy().wait_send()
        dx_copy().wait_recv()

        def drain(k, carry):
            b_copy(k).wait_send()
            return carry

        lax.fori_loop(0, n_chunks, drain, 0)


def run_stack(x_t, dy_t, weights, biases):
    steps, half, _ = x_t.shape
    layers = weights.shape[0] // 2
    rows = 2 * half
    n = steps * rows
    n_chunks = steps // T
    vmem = pl.BlockSpec(memory_space=pltpu.VMEM)
    hbm = pl.BlockSpec(memory_space=pl.ANY)
    bf, f32 = jnp.bfloat16, jnp.float32
    dma = pltpu.SemaphoreType.DMA
    return pl.pallas_call(
        functools.partial(stack_kernel, steps, half, layers),
        out_shape=(jax.ShapeDtypeStruct((layers, 2 * H, G // 2), f32), jax.ShapeDtypeStruct((8, G), f32),
                   jax.ShapeDtypeStruct((steps, half, H), f32)),
        in_specs=[vmem, vmem, hbm, vmem],
        out_specs=(hbm, vmem, vmem),
        scratch_shapes=[
            pltpu.VMEM((layers, 2 * H, G), bf), pltpu.VMEM((layers, G, 2 * H), bf),
            pltpu.VMEM((layers + 1, n, H), bf), pltpu.VMEM((layers, n + rows, H), bf),
            pltpu.VMEM((layers, n, G), f32), pltpu.VMEM((layers, n + rows, H), f32),
            pltpu.VMEM((T * rows, G), f32), pltpu.VMEM((layers, n, G), bf),
            pltpu.VMEM((2, n, H), f32), pltpu.VMEM((steps, half, H), bf),
            pltpu.VMEM((steps, half, H), f32),
            pltpu.VMEM((layers, rows, H), f32), pltpu.VMEM((layers, rows, H), f32),
            pltpu.VMEM((layers, rows, G), f32), pltpu.VMEM((256, 2 * n), bf), pltpu.VMEM((2, 256, G // 2), f32),
            pltpu.VMEM((layers, n, H), bf), pltpu.VMEM((layers, n, H), bf), pltpu.VMEM((layers, n, G // 2), bf),
            dma((layers,)), dma((2,)), dma((2,)), dma((n_chunks,)), dma((n_chunks,)), dma((n_chunks,)), dma((n_chunks,)),
            dma, dma, dma((2,)),
            dma((layers, 2)), dma((layers, 2)), dma((layers, n_chunks)), dma((layers, n_chunks)),
        ],
        compiler_params=pltpu.CompilerParams(collective_id=0, has_side_effects=True, vmem_limit_bytes=67_000_000),
        name="stack",
    )(x_t, dy_t, weights, biases)


BLOCKS = 8
DEPTH = 4
TRIGGER = 2
ORDERS = ((("y", "z1", "z2"),) * BLOCKS,
          (("x", "z1", "z2"),) * BLOCKS,
          (("x", "y", "z2"), ("y", "x", "z2")) * (BLOCKS // 2))


def event_order(layers):
    free = {"x": 0.0, "y": 0.0, "z": 0.0}
    pending = []

    def send(now, c, s, step):
        q = step if step < 3 else 5 - step
        dim = PAIR[c] if step == 6 else ORDERS[c][s][q]
        link = dim[0]
        free[link] = max(now, free[link]) + 0.5 ** q * (1.0 if dim == "z2" else 1.0)
        pending.append((free[link] + 0.5, s, c, step))

    for s in range(DEPTH):
        for c in range(layers):
            send(0.0, c, s, 0)
    order = []
    while pending:
        pending.sort()
        now, s, c, step = pending.pop(0)
        order.append((c, s, step))
        if step < 6:
            send(now, c, s, step + 1)
        if step == TRIGGER and s + DEPTH < BLOCKS:
            send(now, c, s + DEPTH, 0)
    return order


def sum_kernel(layers, dw_in, db_in, dw_out, db_out, loc, land0, land1, land2, dbl, dba,
               loc_sem, put_sem, rs_send, rs_recv, ag_send, ag_recv, c_send, c_recv, db_send, db_recv):
    land = (land0, land1, land2)
    bits, peer, core = chip_map()
    first = core * layers
    block = dw_in.shape[1] // BLOCKS
    width = dw_in.shape[2]

    barrier = pltpu.get_barrier_semaphore()
    for p in peer.values():
        pl.semaphore_signal(barrier, inc=1, device_id=p, device_id_type=MESH)
    pl.semaphore_wait(barrier, len(peer))

    def rows(off, size):
        return pl.ds(pl.multiple_of(off, 8), size)

    def own_cols(c):
        return pl.ds(pl.multiple_of(bits[PAIR[c]] * width, width), width)

    def offset(c, s, steps):
        off = s * block
        for q in range(steps):
            off = off + bits[ORDERS[c][s][q]] * (block >> (q + 1))
        return off

    def local_load(c, s):
        return pltpu.make_async_copy(dw_in.at[c, rows(offset(c, s, 1), block // 2)], loc.at[c, s], loc_sem.at[c, s])

    def reduce_copy(c, s, q):
        dim = ORDERS[c][s][q]
        size = block >> (q + 1)
        if q == 0:
            src = dw_in.at[c, rows(s * block + (1 - bits[dim]) * size, size)]
        else:
            src = land[q - 1].at[c, s, rows((1 - bits[dim]) * size, size)]
        return pltpu.make_async_remote_copy(src_ref=src, dst_ref=land[q].at[c, s], send_sem=rs_send.at[c, s, q],
                                            recv_sem=rs_recv.at[c, s, q], device_id=peer[dim], device_id_type=MESH)

    def put(c, s):
        return pltpu.make_async_copy(land2.at[c, s], dw_out.at[first + c, rows(offset(c, s, 3), block // 8), own_cols(c)],
                                     put_sem.at[c, s])

    def gather_copy(c, s, step):
        q = 5 - step
        dim = PAIR[c] if q < 0 else ORDERS[c][s][q]
        where = dw_out.at[first + c, rows(offset(c, s, q + 1), block >> (q + 1)), own_cols(c)]
        return pltpu.make_async_remote_copy(src_ref=land2.at[c, s] if q == 2 else where, dst_ref=where,
                                            send_sem=ag_send.at[c, s, step - 3], recv_sem=ag_recv.at[c, s, step - 3],
                                            device_id=peer[dim], device_id_type=MESH)

    def core_copy(c, s):
        where = dw_out.at[first + c, rows(s * block, block)]
        return pltpu.make_async_remote_copy(src_ref=where, dst_ref=where, send_sem=c_send.at[c, s],
                                            recv_sem=c_recv.at[c, s], device_id=peer["c"], device_id_type=MESH)

    db_dims = ("x", "y", "z1", "z2")

    def db_copy(p):
        return pltpu.make_async_remote_copy(src_ref=dba.at[p], dst_ref=dbl.at[p], send_sem=db_send.at[p],
                                            recv_sem=db_recv.at[p], device_id=peer[db_dims[p]], device_id_type=MESH)

    def db_core_copy():
        return pltpu.make_async_remote_copy(src_ref=dba.at[4], dst_ref=db_out.at[core], send_sem=db_send.at[4],
                                            recv_sem=db_recv.at[4], device_id=peer["c"], device_id_type=MESH)

    dba[0] = db_in[...]
    db_copy(0).start()
    for s in range(DEPTH):
        for c in range(layers):
            reduce_copy(c, s, 0).start()
    for s in range(BLOCKS):
        for c in range(layers):
            local_load(c, s).start()

    def add(dst, src_of, size):
        def body(i, carry):
            r = pl.ds(pl.multiple_of(i * 8, 8), 8)
            dst[r, :] = dst[r, :] + src_of(i * 8)
            return carry

        lax.fori_loop(0, size // 8, body, 0)

    order = event_order(layers)
    spread = max(1, len(order) // 8)
    for n, (c, s, step) in enumerate(order):
        if step < 3:
            size = block >> (step + 1)
            reduce_copy(c, s, step).wait_recv()
            if step == 0:
                local_load(c, s).wait()
                add(land0.at[c, s], lambda i: loc[c, s, rows(i, 8), :], size)
            else:
                keep = bits[ORDERS[c][s][step]] * size
                add(land[step].at[c, s], lambda i: land[step - 1][c, s, rows(keep + i, 8), :], size)
            if step < 2:
                reduce_copy(c, s, step + 1).start()
            else:
                put(c, s).start()
                gather_copy(c, s, 3).start()
        else:
            if step == 3:
                put(c, s).wait()
            gather_copy(c, s, step).wait_recv()
            if step < 6:
                gather_copy(c, s, step + 1).start()
            else:
                core_copy(c, s).start()
        if step == TRIGGER and s + DEPTH < BLOCKS:
            reduce_copy(c, s + DEPTH, 0).start()
        if n % spread == spread - 1 and n // spread < 4:
            p = n // spread
            db_copy(p).wait_recv()
            dba[p + 1] = dba[p] + dbl[p]
            if p < 3:
                db_copy(p + 1).start()
            else:
                db_core_copy().start()
                db_out[core] = dba[4]

    for s in range(BLOCKS):
        for c in range(layers):
            core_copy(c, s).wait_recv()
            core_copy(c, s).wait_send()
            for q in range(3):
                reduce_copy(c, s, q).wait_send()
            for step in range(3, 7):
                gather_copy(c, s, step).wait_send()
    db_core_copy().wait()
    for p in range(4):
        db_copy(p).wait_send()


def sum_over_chips(dw, db):
    layers, n_rows, n_cols = dw.shape
    block = n_rows // BLOCKS
    f32 = jnp.float32
    vmem = pl.BlockSpec(memory_space=pltpu.VMEM)
    hbm = pl.BlockSpec(memory_space=pl.ANY)
    dma = pltpu.SemaphoreType.DMA
    return pl.pallas_call(
        functools.partial(sum_kernel, layers),
        out_shape=(jax.ShapeDtypeStruct((2 * layers, n_rows, 2 * n_cols), f32), jax.ShapeDtypeStruct((2,) + db.shape, f32)),
        in_specs=[hbm, vmem],
        out_specs=(hbm, vmem),
        scratch_shapes=[
            pltpu.VMEM((layers, BLOCKS, block // 2, n_cols), f32), pltpu.VMEM((layers, BLOCKS, block // 2, n_cols), f32),
            pltpu.VMEM((layers, BLOCKS, block // 4, n_cols), f32), pltpu.VMEM((layers, BLOCKS, block // 8, n_cols), f32),
            pltpu.VMEM((4,) + db.shape, f32), pltpu.VMEM((5,) + db.shape, f32),
            dma((layers, BLOCKS)), dma((layers, BLOCKS)), dma((layers, BLOCKS, 3)), dma((layers, BLOCKS, 3)),
            dma((layers, BLOCKS, 4)), dma((layers, BLOCKS, 4)), dma((layers, BLOCKS)), dma((layers, BLOCKS)),
            dma((5,)), dma((5,)),
        ],
        compiler_params=pltpu.CompilerParams(collective_id=1, has_side_effects=True, vmem_limit_bytes=67_000_000),
        name="sum",
    )(dw, db)


def solution(mesh):
    batch_axes = tuple(mesh.axis_names)

    def device_step(x_in, d_out, weights, biases):
        layers = weights.shape[0] // 2
        dw, db, dx = run_stack(jnp.swapaxes(x_in, 0, 1), jnp.swapaxes(d_out, 0, 1), weights, biases)
        dw_all, db_all = sum_over_chips(dw, db)
        return dw_all, db_all[:, :layers].reshape(biases.shape), jnp.swapaxes(dx, 0, 1)

    return jax.shard_map(device_step, mesh=mesh,
                         in_specs=(P(batch_axes), P(batch_axes), P(), P()),
                         out_specs=(P(), P(), P(batch_axes)), check_vma=False)
```
